32 devices in a mesh: part: 1 (over z), tp: 4 (over y), ep: 8 (over x, core).
Axes of the slice: x: 4, y: 4, z: 1, core: 2. Of those that a mesh axis runs over, the one named last changes fastest.
The devices are a block of a 4x4x8 slice.
Arguments:
- dec_states: bfloat16 [64, 512, 768], P(('part', 'ep'))
- enc_states: bfloat16 [64, 256, 768], P(('part', 'ep'))
- enc_pad: int32 [64, 256], P(('part', 'ep'))
- expert_idx: int32 [64, 512], P(('part', 'ep'))
- self_bias: float32 [12, 512, 512], P('tp')
- gain_self: float32 [768], replicated
- wq_self: bfloat16 [768, 768], P(None, 'tp')
- wk_self: bfloat16 [768, 768], P(None, 'tp')
- wv_self: bfloat16 [768, 768], P(None, 'tp')
- wo_self: bfloat16 [768, 768], P('tp')
- gain_cross: float32 [768], replicated
- wq_cross: bfloat16 [768, 768], P(None, 'tp')
- wk_cross: bfloat16 [768, 768], P(None, 'tp')
- wv_cross: bfloat16 [768, 768], P(None, 'tp')
- wo_cross: bfloat16 [768, 768], P('tp')
- gain_ffn: float32 [768], replicated
- w_router: float32 [768, 128], replicated
- w_in: bfloat16 [128, 768, 3072], P('ep')
- w_out: bfloat16 [128, 3072, 768], P('ep')
Outputs:
- output: bfloat16 [64, 512, 768], P(('part', 'ep'))
All inputs are finite; a program needn't handle non-finite values.
Results may differ from the reference program's by a relative error of at most 0.02.
Values are sent between devices in bfloat16 or wider.
A program may use at most 768 MiB of HBM per device.

```python
import math
import jax
import jax.numpy as jnp
from jax import lax

D_MODEL = 768
NUM_HEADS = 12
HEAD_DIM = 64
D_FF = 3072
EXPERTS = 128
GROUPS = 8
BATCH_DEV = 8
DEC_LEN = 512
ENC_LEN = 256

GROUP_BATCH = GROUPS * BATCH_DEV
TOKENS = BATCH_DEV * DEC_LEN
CAPACITY = (5 * TOKENS + 4 * EXPERTS - 1) // (4 * EXPERTS)
HIDDEN = NUM_HEADS * HEAD_DIM
EPSILON = 1e-6
NEG_LARGE = -1e30


def normal_draw(key, shape, scale):
    return jax.random.normal(key, shape, jnp.float32) * scale


def draw_expert_in(key):
    return normal_draw(key, (D_MODEL, D_FF), D_MODEL ** -0.5).astype(jnp.bfloat16)


def draw_expert_out(key):
    return normal_draw(key, (D_FF, D_MODEL), 0.4 * EXPERTS * D_FF ** -0.5).astype(jnp.bfloat16)


def relative_class(length):
    rel_pos = jnp.arange(length)[:, None] - jnp.arange(length)[None, :]
    distance = jnp.maximum(rel_pos, 0)
    far_class = jnp.full(distance.shape, 16, jnp.int32)
    for step_idx in range(1, 16):
        threshold = int(math.ceil(16.0 * 8.0 ** (step_idx / 16.0)))
        far_class = far_class + (distance >= threshold).astype(jnp.int32)
    return jnp.where(distance < 16, distance, far_class)


def draw_layout(key):
    route_keys = jax.random.split(key, 5)
    first_pick = jax.random.randint(route_keys[0], (GROUPS, TOKENS), 0, EXPERTS)
    second_pick = jax.random.randint(route_keys[1], (GROUPS, TOKENS), 0, EXPERTS)
    coin_flip = jax.random.randint(route_keys[2], (GROUPS, TOKENS), 0, 2)
    skewed = jnp.where(coin_flip == 1, first_pick, jnp.minimum(first_pick, second_pick))
    hot_expert = jax.random.randint(route_keys[3], (GROUPS, 1), 0, EXPERTS)
    local_pos = jnp.arange(TOKENS)[None, :]
    expert_idx = jnp.where(local_pos <= CAPACITY, hot_expert, skewed).reshape(GROUP_BATCH, DEC_LEN).astype(jnp.int32)
    pad_min = ENC_LEN // 10
    pad_max = 2 * ENC_LEN // 5
    pad_len = jax.random.randint(route_keys[4], (GROUP_BATCH,), pad_min, pad_max + 1)
    row_ids = jnp.arange(GROUP_BATCH)
    pad_len = jnp.where(row_ids == 0, pad_max, jnp.where(row_ids == 1, pad_min, pad_len))
    enc_pad = (jnp.arange(ENC_LEN)[None, :] >= ENC_LEN - pad_len[:, None]).astype(jnp.int32)
    return enc_pad, expert_idx


def setup_inputs(seed: int = 0, part: int = 0) -> dict:
    base_key = jax.random.key(seed)
    part_keys = jax.random.split(jax.random.fold_in(base_key, part), 3)
    shared_keys = jax.random.split(jax.random.fold_in(base_key, 1000003), 16)
    enc_pad, expert_idx = draw_layout(part_keys[2])
    scale_in = D_MODEL ** -0.5
    scale_query = 2.0 * (D_MODEL * HEAD_DIM) ** -0.5
    scale_out = HIDDEN ** -0.5
    qkv_shape = (D_MODEL, HIDDEN)
    return {
        'dec_states': normal_draw(part_keys[0], (GROUP_BATCH, DEC_LEN, D_MODEL), 0.5).astype(jnp.bfloat16),
        'enc_states': normal_draw(part_keys[1], (GROUP_BATCH, ENC_LEN, D_MODEL), 1.0).astype(jnp.bfloat16),
        'enc_pad': enc_pad,
        'expert_idx': expert_idx,
        'self_bias': normal_draw(shared_keys[0], (NUM_HEADS, 32), 1.0)[:, relative_class(DEC_LEN)],
        'gain_self': jax.random.uniform(shared_keys[1], (D_MODEL,), jnp.float32, 0.25, 1.75),
        'wq_self': normal_draw(shared_keys[2], qkv_shape, scale_query).astype(jnp.bfloat16),
        'wk_self': normal_draw(shared_keys[3], qkv_shape, scale_in).astype(jnp.bfloat16),
        'wv_self': normal_draw(shared_keys[4], qkv_shape, scale_in).astype(jnp.bfloat16),
        'wo_self': normal_draw(shared_keys[5], (HIDDEN, D_MODEL), scale_out).astype(jnp.bfloat16),
        'gain_cross': jax.random.uniform(shared_keys[6], (D_MODEL,), jnp.float32, 0.25, 1.75),
        'wq_cross': normal_draw(shared_keys[7], qkv_shape, scale_query).astype(jnp.bfloat16),
        'wk_cross': normal_draw(shared_keys[8], qkv_shape, scale_in).astype(jnp.bfloat16),
        'wv_cross': normal_draw(shared_keys[9], qkv_shape, scale_in).astype(jnp.bfloat16),
        'wo_cross': normal_draw(shared_keys[10], (HIDDEN, D_MODEL), scale_out).astype(jnp.bfloat16),
        'gain_ffn': jax.random.uniform(shared_keys[11], (D_MODEL,), jnp.float32, 0.25, 1.75),
        'w_router': normal_draw(shared_keys[12], (D_MODEL, EXPERTS), scale_in),
        'w_in': lax.map(draw_expert_in, jax.random.split(shared_keys[13], EXPERTS)),
        'w_out': lax.map(draw_expert_out, jax.random.split(shared_keys[14], EXPERTS)),
    }


def rms_norm(states, gain_vec):
    upcast = states.astype(jnp.float32)
    mean_sq = jnp.mean(upcast * upcast, axis=-1, keepdims=True)
    return (upcast * lax.rsqrt(mean_sq + EPSILON) * gain_vec).astype(jnp.bfloat16)


def project_heads(states, weight):
    projected = jnp.dot(states.reshape(-1, D_MODEL), weight, preferred_element_type=jnp.float32)
    return projected.astype(jnp.bfloat16).reshape(states.shape[0], states.shape[1], NUM_HEADS, HEAD_DIM)


def output_sum(context, weight):
    return jnp.dot(context.reshape(-1, HIDDEN), weight, preferred_element_type=jnp.float32)


def residual_add(states, update):
    return (states.astype(jnp.float32) + update.reshape(states.shape)).astype(jnp.bfloat16)


def softmax_mix(queries, key_heads, values, bias_mask):
    scores = jnp.einsum('qhe,khe->hqk', queries.astype(jnp.float32), key_heads.astype(jnp.float32)) + bias_mask
    weights = jax.nn.softmax(scores, axis=-1).astype(jnp.bfloat16)
    return jnp.einsum('hqk,khe->qhe', weights.astype(jnp.float32), values.astype(jnp.float32)).astype(jnp.bfloat16)


def expert_ffn(operands):
    inputs, first_w, second_w = operands
    hidden = jnp.maximum(jnp.dot(inputs, first_w, preferred_element_type=jnp.float32), 0.0).astype(jnp.bfloat16)
    return jnp.dot(hidden, second_w, preferred_element_type=jnp.float32).astype(jnp.bfloat16)


def reference(dec_states, enc_states, enc_pad, expert_idx, self_bias, gain_self, wq_self, wk_self, wv_self, wo_self, gain_cross, wq_cross, wk_cross, wv_cross, wo_cross, gain_ffn, w_router, w_in, w_out):
    row_ids = jnp.arange(DEC_LEN)[:, None]
    col_ids = jnp.arange(DEC_LEN)[None, :]
    causal_bias = jnp.where(col_ids <= row_ids, self_bias, NEG_LARGE)

    def self_seq(operands):
        return softmax_mix(operands[0], operands[1], operands[2], causal_bias)

    def cross_seq(operands):
        return softmax_mix(operands[0], operands[1], operands[2], operands[3])

    normed = rms_norm(dec_states, gain_self)
    context = lax.map(self_seq, (project_heads(normed, wq_self), project_heads(normed, wk_self), project_heads(normed, wv_self)))
    after_self = residual_add(dec_states, output_sum(context, wo_self))

    pad_bias = jnp.where(enc_pad == 0, 0.0, NEG_LARGE).astype(jnp.float32)[:, None, None, :]
    normed = rms_norm(after_self, gain_cross)
    context = lax.map(cross_seq, (project_heads(normed, wq_cross), project_heads(enc_states, wk_cross), project_heads(enc_states, wv_cross), pad_bias))
    after_cross = residual_add(after_self, output_sum(context, wo_cross))

    normed = rms_norm(after_cross, gain_ffn).reshape(GROUPS, TOKENS, D_MODEL)
    logits = jnp.dot(normed.reshape(-1, D_MODEL).astype(jnp.float32), w_router)
    router_prob = jax.nn.softmax(logits, axis=-1).reshape(GROUPS, TOKENS, EXPERTS)
    choice = expert_idx.reshape(GROUPS, TOKENS)
    one_hot = (choice[:, :, None] == jnp.arange(EXPERTS)[None, None, :]).astype(jnp.int32)
    gate_prob = jnp.sum(router_prob * one_hot, axis=-1)
    position = jnp.sum((jnp.cumsum(one_hot, axis=1) - 1) * one_hot, axis=-1)
    is_kept = position < CAPACITY
    slot_count = EXPERTS * CAPACITY
    slot_id = jnp.where(is_kept, choice * CAPACITY + position, slot_count)
    target = jnp.arange(GROUPS)[:, None] * (slot_count + 1) + slot_id
    buffers = jnp.zeros((GROUPS * (slot_count + 1), D_MODEL), jnp.bfloat16)
    buffers = buffers.at[target.reshape(-1)].set(normed.reshape(-1, D_MODEL))
    buffers = buffers.reshape(GROUPS, slot_count + 1, D_MODEL)[:, :slot_count]
    per_expert = jnp.transpose(buffers.reshape(GROUPS, EXPERTS, CAPACITY, D_MODEL), (1, 0, 2, 3)).reshape(EXPERTS, GROUPS * CAPACITY, D_MODEL)
    expert_out = lax.map(expert_ffn, (per_expert, w_in, w_out))
    expert_out = jnp.transpose(expert_out.reshape(EXPERTS, GROUPS, CAPACITY, D_MODEL), (1, 0, 2, 3)).reshape(GROUPS * slot_count, D_MODEL)
    source = jnp.arange(GROUPS)[:, None] * slot_count + jnp.where(is_kept, slot_id, 0)
    picked = expert_out[source.reshape(-1)].astype(jnp.float32).reshape(GROUPS, TOKENS, D_MODEL)
    moe_out = (gate_prob * is_kept)[:, :, None] * picked
    result = after_cross.reshape(GROUPS, TOKENS, D_MODEL).astype(jnp.float32) + moe_out
    return result.astype(jnp.bfloat16).reshape(GROUP_BATCH, DEC_LEN, D_MODEL)
```

```python
import functools

import jax
import jax.numpy as jnp
from jax import lax
from jax.experimental import pallas as pl
from jax.experimental.pallas import tpu as pltpu
from jax.sharding import PartitionSpec as P

EPSILON = 1e-6
NEG_LARGE = -1e30
MESH = pl.DeviceIdType.MESH
BF16 = jnp.bfloat16
F32 = jnp.float32
LANES = 128
VMEM_LIMIT = 67043328


def rms_norm(upcast, gain_vec):
    mean_sq = jnp.mean(upcast * upcast, axis=-1, keepdims=True)
    return (upcast * lax.rsqrt(mean_sq + EPSILON) * gain_vec).astype(BF16)


def dot(a, b):
    return jnp.dot(a, b, preferred_element_type=F32)


def dot_nt(a, b):
    return lax.dot_general(a, b, (((1,), (1,)), ((), ())), preferred_element_type=F32)


def softmax(scores):
    exps = jnp.exp(scores - jnp.max(scores, axis=-1, keepdims=True))
    return (exps * (1.0 / jnp.sum(exps, axis=-1, keepdims=True))).astype(BF16)


def low_lanes(rows):
    return lax.broadcasted_iota(jnp.int32, (rows, LANES), 1) < LANES // 2


def pack_qkv(w_query, w_key, w_value):
    half, full = LANES // 2, LANES
    blank = jnp.zeros((w_query.shape[0], half), w_query.dtype)
    return jnp.concatenate([w_query, blank, w_key[:, :full], w_value[:, :full], w_key[:, full:], w_value[:, full:]], axis=1)


def pack_out(w_output):
    blank = jnp.zeros((LANES // 2, w_output.shape[1]), w_output.dtype)
    return jnp.concatenate([w_output[:LANES], blank, w_output[LANES:]], axis=0)


def remote(src, dst, send_sem, recv_sem, **device):
    return pltpu.make_async_remote_copy(src_ref=src, dst_ref=dst, send_sem=send_sem, recv_sem=recv_sem, device_id=device, device_id_type=MESH)


def barrier(devices):
    sem = pltpu.get_barrier_semaphore()
    for device in devices:
        pl.semaphore_signal(sem, inc=1, device_id=device, device_id_type=MESH)
    pl.semaphore_wait(sem, len(devices))


def self_kernel(tp, ep, dec_ref, gain_ref, w_ref, bias_ref, wq_ref, wo_ref, ctx_ref, wq_all, wo_all, dec_buf, head_buf, ctx_buf, relay, wq_buf, wo_buf, dec_sem, load_sem, ctx_send, ctx_recv, own_sem, wy_send, wy_recv, wx_send, wx_recv, wd_send, wd_recv):
    t, e = lax.axis_index('tp'), lax.axis_index('ep')
    right, left, across = lax.rem(t + 1, tp), lax.rem(t + tp - 1, tp), lax.rem(t + 2, tp)
    x_right, x_left = lax.rem(e + 2, ep), lax.rem(e + ep - 2, ep)
    core, x = lax.rem(e, 2), e // 2
    x_pos_left, x_pos_right, x_across = x_left // 2, x_right // 2, lax.rem(x + 2, ep // 2)
    partner = e + 1 - 2 * core
    mate = 1 - core
    seqs, length = dec_ref.shape[0], dec_ref.shape[1]
    per = seqs // tp
    heads = bias_ref.shape[0]
    loads = [pltpu.make_async_copy(wq_ref, wq_buf, load_sem.at[0]), pltpu.make_async_copy(wo_ref, wo_buf, load_sem.at[1])]
    for load in loads:
        load.start()

    def seq_at(k):
        off = jnp.where(k < per, 2, jnp.where(k < 2 * per, 1, jnp.where(k < 3 * per, 3, 0)))
        return per * lax.rem(t + off, tp) + lax.rem(k, per)

    def dec_load(k):
        return pltpu.make_async_copy(dec_ref.at[seq_at(k)], dec_buf.at[lax.rem(k, 2)], dec_sem.at[lax.rem(k, 2)])

    dec_load(0).start()
    barrier([{'tp': right}, {'tp': left}, {'ep': x_right}, {'ep': x_left}, {'ep': partner}])
    for load in loads:
        load.wait()
    own_w = [pltpu.make_async_copy(wq_buf, wq_all.at[t], load_sem.at[0]), pltpu.make_async_copy(wo_buf, wo_all.at[t], load_sem.at[1])]
    for load in own_w:
        load.start()
    bufs, alls = (wq_buf, wo_buf), (wq_all, wo_all)

    def wy_own(a, side):
        return remote(bufs[a].at[core, x], alls[a].at[t, core, x], wy_send.at[a, side], wy_recv.at[a, side], tp=(right, left)[side])

    def wy_forward(a):
        src = alls[a].at[(left, right)[a], core, x]
        return remote(src, src, wy_send.at[a, 2], wy_recv.at[a, 2], tp=(right, left)[a])

    def wx_own(a, which, side):
        src = alls[a].at[(left, right, across)[which], core, x]
        return remote(src, src, wx_send.at[a, which, side], wx_recv.at[a, which, side], ep=(x_right, x_left)[side])

    def wx_forward(a, which):
        src = alls[a].at[(left, right, across)[which], core, (x_pos_left, x_pos_right)[a]]
        return remote(src, src, wx_send.at[a, which, 2], wx_recv.at[a, which, 2], ep=(x_right, x_left)[a])

    def wd(a, which):
        src = alls[a].at[(left, right, across)[which], core]
        return remote(src, src, wd_send.at[a, which], wd_recv.at[a, which], ep=partner)

    def y_stage():
        for a in (0, 1):
            for side in (0, 1):
                wy_own(a, side).wait_recv()
            wy_forward(a).start()
        for which in (0, 1):
            for a in (0, 1):
                for side in (0, 1):
                    wx_own(a, which, side).start()

    def across_stage():
        for a in (0, 1):
            wy_forward(a).wait_recv()
            for side in (0, 1):
                wx_own(a, 2, side).start()

    def x_stage(whichs):
        for which in whichs:
            for a in (0, 1):
                for side in (0, 1):
                    wx_own(a, which, side).wait_recv()
                wx_forward(a, which).start()

    def d_stage(whichs):
        for which in whichs:
            for a in (0, 1):
                wx_forward(a, which).wait_recv()
                wd(a, which).start()

    for a in (0, 1):
        for side in (0, 1):
            wy_own(a, side).start()

    def to_side(i, side):
        return remote(ctx_buf.at[per * (1 + side) + i], ctx_ref.at[t, i], ctx_send.at[side, i], ctx_recv.at[side, i], tp=(right, left)[side])

    def to_relay(side):
        return remote(ctx_buf.at[side], relay.at[side], ctx_send.at[2, side], ctx_recv.at[2, side], tp=(right, left)[side])

    def from_relay(side):
        return remote(relay.at[side], ctx_ref.at[(left, right)[side], side], ctx_send.at[3, side], ctx_recv.at[3, side], tp=(right, left)[side])

    def own_ctx(i):
        return pltpu.make_async_copy(ctx_buf.at[3 * per + i], ctx_ref.at[t, i], own_sem.at[i])

    block = length // 2

    def body(k, carry):
        dec_load(k).wait()

        @pl.when(k + 1 < seqs)
        def _():
            dec_load(k + 1).start()

        normed = rms_norm(dec_buf[lax.rem(k, 2)].astype(F32), gain_ref[...])
        low = low_lanes(length)
        pair = dot(normed, w_ref[:, :2 * LANES])
        q01 = pair[:, :LANES]
        head_buf[0] = jnp.where(low, q01, 0.0).astype(BF16)
        head_buf[1] = jnp.where(low, 0.0, q01).astype(BF16)
        head_buf[2] = pair[:, LANES:].astype(BF16)
        rest = dot(normed, w_ref[:, 2 * LANES:])
        for piece in range(3):
            head_buf[3 + piece] = rest[:, piece * LANES:(piece + 1) * LANES].astype(BF16)
        low_half = low_lanes(block)
        for half in (0, 1):
            rows = slice(half * block, (half + 1) * block)
            keys = slice(0, (half + 1) * block)
            row_ids = half * block + lax.broadcasted_iota(jnp.int32, (block, (half + 1) * block), 0)
            col_ids = lax.broadcasted_iota(jnp.int32, (block, (half + 1) * block), 1)
            mixed = []
            for head in range(heads):
                key_at, value_at = (3, 4) if head < 2 else (5, 5)
                scores = dot_nt(head_buf[head, rows], head_buf[key_at, keys]) + bias_ref[head, rows, keys]
                scores = jnp.where(col_ids <= row_ids, scores, NEG_LARGE)
                mixed.append(dot(softmax(scores), head_buf[value_at, keys]))
            ctx_buf[k, rows, :LANES] = jnp.where(low_half, mixed[0], mixed[1]).astype(BF16)
            ctx_buf[k, rows, LANES:] = mixed[2].astype(BF16)

        @pl.when(k == 0)
        def _():
            to_relay(0).start()
            y_stage()

        @pl.when(k == 1)
        def _():
            to_relay(1).start()
            across_stage()

        for side in (0, 1):
            for i in range(per):
                @pl.when(k == per * (1 + side) + i)
                def _(side=side, i=i):
                    to_side(i, side).start()

        @pl.when(k == 2)
        def _():
            to_relay(0).wait_recv()
            from_relay(0).start()

        @pl.when(k == 3)
        def _():
            to_relay(1).wait_recv()
            from_relay(1).start()

        @pl.when(k == 4)
        def _():
            x_stage((0, 1))

        @pl.when(k == 6)
        def _():
            x_stage((2,))
            d_stage((0, 1))

        for i in range(per):
            @pl.when(k == 3 * per + i)
            def _(i=i):
                own_ctx(i).start()

        return carry

    lax.fori_loop(0, seqs, body, 0)
    d_stage((2,))
    for load in own_w:
        load.wait()
    for i in range(per):
        own_ctx(i).wait()
    for side in (0, 1):
        for i in range(per):
            to_side(i, side).wait()
        to_relay(side).wait_send()
        from_relay(side).wait()
    for a in (0, 1):
        for side in (0, 1):
            wy_own(a, side).wait_send()
        wy_forward(a).wait_send()
        for which in range(3):
            for side in (0, 1):
                wx_own(a, which, side).wait_send()
            wx_forward(a, which).wait_send()
            wd(a, which).wait()


def cross_kernel(tp, ep, cap, experts, ctx_ref, w_ref, wo_ref, dec_ref, enc_ref, pad_ref, gain_cross_ref, gain_ffn_ref, router_ref, idx_row_ref, idx_col_ref, y2_ref, send_ref, gate_ref, slot_ref, dec_buf, enc_buf, y1_buf, x_buf, q_buf, kv_buf, acc_buf, y2_buf, route_buf, tri_buf, key_buf, dec_sem, enc_sem, y_send, y_recv, out_sem):
    t = lax.axis_index('tp')
    right, left, across = lax.rem(t + 1, tp), lax.rem(t + tp - 1, tp), lax.rem(t + 2, tp)
    seqs, length, width = y2_buf.shape
    per = seqs // tp
    span = experts // ep
    share = span // tp
    wo_rows = 2 * LANES

    def load(i):
        return (pltpu.make_async_copy(dec_ref.at[per * t + i], dec_buf.at[i], dec_sem.at[i]), pltpu.make_async_copy(enc_ref.at[per * t + i], enc_buf.at[i], enc_sem.at[i]))

    for i in range(per):
        for copy in load(i):
            copy.start()
    barrier([{'tp': right}, {'tp': left}])

    def own(i, side):
        src = y2_buf.at[per * t + i]
        return remote(src, src, y_send.at[side, i], y_recv.at[side, i], tp=(right, left)[side])

    def forward(side):
        src = y2_buf.at[per * (left, right)[side] + side]
        return remote(src, src, y_send.at[2, side], y_recv.at[2, side], tp=(right, left)[side])

    def write(s):
        return pltpu.make_async_copy(y2_buf.at[s], y2_ref.at[s], out_sem.at[s])

    low = low_lanes(length)

    def attend(i, carry):
        for copy in load(i):
            copy.wait()
        total = dec_buf[i].astype(F32)
        for row in range(tp):
            total = total + dot(ctx_ref[row, i], wo_ref[row, :wo_rows])
        y1 = total.astype(BF16)
        y1_buf[...] = y1
        x_buf[...] = rms_norm(y1.astype(F32), gain_cross_ref[...])
        acc_buf[...] = jnp.zeros_like(acc_buf)
        pad_bias = jnp.where(pad_ref[pl.ds(per * t + i, 1), :] == 0, 0.0, NEG_LARGE)

        def per_row(row, inner):
            pair = dot(x_buf[...], w_ref[row, :, :2 * LANES])
            q01 = pair[:, :LANES]
            q_buf[0] = jnp.where(low, q01, 0.0).astype(BF16)
            q_buf[1] = jnp.where(low, 0.0, q01).astype(BF16)
            q_buf[2] = pair[:, LANES:].astype(BF16)
            rest = dot(enc_buf[i], w_ref[row, :, 2 * LANES:])
            for piece in range(3):
                kv_buf[piece] = rest[:, piece * LANES:(piece + 1) * LANES].astype(BF16)
            mixed = []
            for head in range(3):
                key_at, value_at = (0, 1) if head < 2 else (2, 2)
                scores = dot_nt(q_buf[head], kv_buf[key_at]) + pad_bias
                mixed.append(dot(softmax(scores), kv_buf[value_at]))
            c01 = jnp.where(low, mixed[0], mixed[1]).astype(BF16)
            acc_buf[...] += dot(c01, wo_ref[row, wo_rows:wo_rows + LANES]) + dot(mixed[2].astype(BF16), wo_ref[row, wo_rows + LANES:])
            return inner

        lax.fori_loop(0, tp, per_row, 0)
        y2_buf[per * t + i] = (y1_buf[...].astype(F32) + acc_buf[...]).astype(BF16)
        for step in range(per):
            @pl.when(i == step)
            def _(step=step):
                for side in (0, 1):
                    own(step, side).start()
        write(per * t + i).start()
        return carry

    lax.fori_loop(0, per, attend, 0)

    w_full = router_ref[...]
    w_high = w_full.astype(BF16)
    w_rest = w_full - w_high.astype(F32)
    w_mid = w_rest.astype(BF16)
    route_buf[:, :experts] = w_high
    route_buf[:, experts:2 * experts] = w_mid
    route_buf[:, 2 * experts:] = (w_rest - w_mid.astype(F32)).astype(BF16)
    row_ids = lax.broadcasted_iota(jnp.int32, (length, length), 0)
    col_ids = lax.broadcasted_iota(jnp.int32, (length, length), 1)
    tri_buf[0] = jnp.where(col_ids <= row_ids, 1.0, 0.0).astype(BF16)
    tri_buf[1] = jnp.where(row_ids <= col_ids, 1.0, 0.0).astype(BF16)
    lane_e = lax.broadcasted_iota(jnp.int32, (length, experts), 1)
    sub_e = lax.broadcasted_iota(jnp.int32, (experts, length), 0)
    lane_s = lax.broadcasted_iota(jnp.int32, idx_col_ref.shape, 1)
    slot_ref[...] = jnp.zeros_like(slot_ref)
    gate_ref[...] = jnp.zeros_like(gate_ref)

    def choice_col(s):
        return jnp.sum(jnp.where(lane_s == s, idx_col_ref[...], 0), axis=1, keepdims=True)

    def place(s, carry):
        base_row, base_col = carry
        col = choice_col(s)
        hot = jnp.where(lane_e == col, 1.0, 0.0)
        count = dot(tri_buf[0], hot.astype(BF16)) + base_row
        pos = jnp.sum(hot * count, axis=1, keepdims=True) - 1.0
        slot = jnp.where(pos < cap, col * cap + pos.astype(jnp.int32), -1)
        slot_ref[...] += jnp.where(lane_s == s, slot, 0)
        row = idx_row_ref[pl.ds(s, 1), :]
        hot_t = jnp.where(sub_e == row, 1.0, 0.0)
        count_t = dot(hot_t.astype(BF16), tri_buf[1]) + base_col
        pos_t = jnp.sum(hot_t * count_t, axis=0, keepdims=True) - 1.0
        mine = (pos_t < cap) & (lax.rem(row // share, tp) == t)
        key_buf[pl.ds(s, 1), :] = jnp.where(mine, (row // span) * (share * cap) + lax.rem(row, share) * cap + pos_t.astype(jnp.int32), -1)
        return count[length - 1:, :], count_t[:, length - 1:]

    lax.fori_loop(0, seqs, place, (jnp.zeros((1, experts), F32), jnp.zeros((experts, 1), F32)))
    send_ref[...] = jnp.zeros_like(send_ref)
    chunk = share * cap

    def consume(n, carry):
        near = jnp.where(lax.rem(n, 2) == 0, left, right)
        row = jnp.where(n < per, t, jnp.where(n < 3 * per, near, across))
        half = jnp.where(n < per, n, jnp.where(n < 3 * per, lax.rem(n // 2 + 1, 2), lax.rem(n, 2)))
        s = per * row + half

        @pl.when(n == 2)
        def _():
            own(0, 0).wait_recv()
            forward(0).start()

        @pl.when(n == 3)
        def _():
            own(0, 1).wait_recv()

        @pl.when(n == 4)
        def _():
            own(1, 0).wait_recv()
            own(1, 1).wait_recv()
            forward(1).start()

        @pl.when(n == 6)
        def _():
            forward(0).wait_recv()

        @pl.when(n == 7)
        def _():
            forward(1).wait_recv()

        @pl.when(n >= per)
        def _():
            write(s).start()

        normed = rms_norm(y2_buf[s].astype(F32), gain_ffn_ref[...])
        x_buf[...] = normed
        parts = dot(normed, route_buf[...])
        logits = parts[:, :experts] + (parts[:, experts:2 * experts] + parts[:, 2 * experts:])
        exps = jnp.exp(logits - jnp.max(logits, axis=-1, keepdims=True))
        picked = jnp.sum(jnp.where(lane_e == choice_col(s), exps, 0.0), axis=-1, keepdims=True)
        gate_ref[...] += jnp.where(lane_s == s, picked / jnp.sum(exps, axis=-1, keepdims=True), 0.0)
        key = key_buf[pl.ds(s, 1), :]

        def dispatch(d, inner):
            rows = pl.ds(d * chunk, chunk)
            hot = jnp.where(lax.broadcasted_iota(jnp.int32, (chunk, length), 0) + d * chunk == key, 1.0, 0.0).astype(BF16)
            send_ref[rows, :] = (send_ref[rows, :].astype(F32) + dot(hot, x_buf[...])).astype(BF16)
            return inner

        lax.fori_loop(0, ep, dispatch, 0)
        return carry

    lax.fori_loop(0, seqs, consume, 0)
    for s in range(seqs):
        write(s).wait()
    for side in (0, 1):
        for i in range(per):
            own(i, side).wait_send()
        forward(side).wait_send()


def expert_kernel(tp, ep, cap, send_ref, w_in_ref, w_out_ref, y2_ref, gate_ref, slot_ref, out_ref, got, staged, out_stage, out_buf, all_buf, acc_buf, y2_buf, w_in_buf, w_out_buf, xd_send, xd_recv, xr_send, xr_recv, y_send, y_recv, w_sem, own_sem, y2_sem, out_sem):
    t, e = lax.axis_index('tp'), lax.axis_index('ep')
    right, left, across = lax.rem(t + 1, tp), lax.rem(t + tp - 1, tp), lax.rem(t + 2, tp)
    seqs, length, width = y2_buf.shape
    share = staged.shape[0]
    pairs = got.shape[1]
    in_pair = share // pairs
    rows2 = in_pair * cap
    ff = w_in_buf.shape[2]
    barrier([{'tp': right}, {'tp': left}] + [{'ep': lax.rem(e + o, ep)} for o in range(1, ep)])

    def dispatch(o, p):
        return remote(send_ref.at[lax.rem(e + o, ep), p], got.at[e, p], xd_send.at[o, p], xd_recv.at[o, p], ep=lax.rem(e + o, ep))

    def give_back(o, p):
        return remote(out_buf.at[p, lax.rem(e + o, ep)], all_buf.at[t, p, e], xr_send.at[o, p], xr_recv.at[o, p], ep=lax.rem(e + o, ep))

    def dispatch_in(o, p):
        return remote(send_ref.at[0, p], got.at[lax.rem(e + ep - o, ep), p], xd_send.at[o, p], xd_recv.at[o, p], ep=lax.rem(e + o, ep))

    def give_in(o, p):
        return remote(out_buf.at[p, 0], all_buf.at[t, p, lax.rem(e + ep - o, ep)], xr_send.at[o, p], xr_recv.at[o, p], ep=lax.rem(e + o, ep))

    def own_dispatch(p):
        return pltpu.make_async_copy(send_ref.at[e, p], got.at[e, p], own_sem.at[p])

    def weights(j):
        return (pltpu.make_async_copy(w_in_ref.at[share * t + j], w_in_buf.at[j % 2], w_sem.at[0, j % 2]), pltpu.make_async_copy(w_out_ref.at[share * t + j], w_out_buf.at[j % 2], w_sem.at[1, j % 2]))

    order = (4, 2, 6, 3, 5, 1, 7)
    for p in range(pairs):
        for o in order:
            dispatch(o, p).start()
        own_dispatch(p).start()
    for j in (0, 1):
        for copy in weights(j):
            copy.start()
    y2_load = pltpu.make_async_copy(y2_ref, y2_buf, y2_sem)
    y2_load.start()
    acc_buf[...] = jnp.zeros_like(acc_buf)

    def share_out(p, side):
        src = all_buf.at[t, p]
        return remote(src, src, y_send.at[side, p], y_recv.at[side, p], tp=(right, left)[side])

    def pass_on(p, side):
        src = all_buf.at[(left, right)[side], p, pl.ds(side * (ep // 2), ep // 2)]
        return remote(src, src, y_send.at[2 + side, p], y_recv.at[2 + side, p], tp=(right, left)[side])

    def came(row, p, side):
        dst = all_buf.at[row, p]
        return remote(dst, dst, y_send.at[side, p], y_recv.at[side, p], tp=right)

    def came_on(p, side):
        dst = all_buf.at[across, p, pl.ds(side * (ep // 2), ep // 2)]
        return remote(dst, dst, y_send.at[2 + side, p], y_recv.at[2 + side, p], tp=right)

    lane_s = lax.broadcasted_iota(jnp.int32, slot_ref.shape, 1)

    def mix(row, p):
        def chunk(s, carry):
            slot = jnp.sum(jnp.where(lane_s == s, slot_ref[...], 0), axis=1, keepdims=True)
            hit = (slot >= 0) & (lax.rem(slot // rows2, tp * pairs) == row * pairs + p)
            key = jnp.where(hit, (slot // (rows2 * pairs * tp)) * rows2 + lax.rem(slot, rows2), -1)
            hot = jnp.where(lax.broadcasted_iota(jnp.int32, (length, ep * rows2), 1) == key, 1.0, 0.0).astype(BF16)
            acc_buf[s] = (acc_buf[s].astype(F32) + dot(hot, all_buf[row, p].reshape(ep * rows2, width))).astype(BF16)
            return carry

        lax.fori_loop(0, seqs, chunk, 0)

    for p in range(pairs):
        own_dispatch(p).wait()
        for o in range(1, ep):
            dispatch_in(o, p).wait_recv()

        def unpack(g, carry):
            block = got[g, p].astype(F32)
            for jj in range(in_pair):
                staged[p * in_pair + jj, pl.ds(pl.multiple_of(g * cap, 8), cap), :] = block[jj * cap:(jj + 1) * cap]
            return carry

        lax.fori_loop(0, ep, unpack, 0)
        for jj in range(in_pair):
            j = p * in_pair + jj
            for copy in weights(j):
                copy.wait()
            inputs = staged[j].astype(BF16)
            staged[j] = jnp.zeros_like(staged[j])

            def ffn(c, carry):
                cols = pl.ds(pl.multiple_of(c * width, LANES), width)
                hidden = jnp.maximum(dot(inputs, w_in_buf[j % 2, :, cols]), 0.0).astype(BF16)
                staged[j] += dot(hidden, w_out_buf[j % 2, cols, :])
                return carry

            lax.fori_loop(0, ff // width, ffn, 0)
            if j + 2 < share:
                for copy in weights(j + 2):
                    copy.start()

        def repack(g, carry):
            for jj in range(in_pair):
                out_stage[pl.ds(jj * cap, cap), :] = staged[p * in_pair + jj, pl.ds(pl.multiple_of(g * cap, 8), cap), :]
            out_buf[p, g] = out_stage[...].astype(BF16)
            return carry

        lax.fori_loop(0, ep, repack, 0)
        for o in order:
            give_back(o, p).start()
        all_buf[t, p, e] = out_buf[p, e]

    for p in range(pairs):
        for o in range(1, ep):
            give_in(o, p).wait_recv()
        for side in (0, 1):
            share_out(p, side).start()
        if p == 0:
            mix(t, p)
    mix(t, 1)
    for p in range(pairs):
        came(left, p, 0).wait_recv()
        pass_on(p, 0).start()
        came(right, p, 1).wait_recv()
        pass_on(p, 1).start()
        mix(left, p)
        mix(right, p)
    y2_load.wait()
    came_on(0, 0).wait_recv()
    came_on(0, 1).wait_recv()
    mix(across, 0)
    came_on(1, 0).wait_recv()
    came_on(1, 1).wait_recv()
    mix(across, 1)

    def write(s):
        return pltpu.make_async_copy(y2_buf.at[s], out_ref.at[s], out_sem.at[s])

    def finish(s, carry):
        gate = jnp.sum(jnp.where(lane_s == s, gate_ref[...], 0.0), axis=1, keepdims=True)
        y2_buf[s] = (y2_buf[s].astype(F32) + gate * acc_buf[s].astype(F32)).astype(BF16)
        write(s).start()
        return carry

    lax.fori_loop(0, seqs, finish, 0)
    for s in range(seqs):
        write(s).wait()
    for p in range(pairs):
        for o in range(1, ep):
            dispatch(o, p).wait_send()
            give_back(o, p).wait_send()
        for side in (0, 1):
            share_out(p, side).wait_send()
            pass_on(p, side).wait_send()


def any_spec():
    return pl.BlockSpec(memory_space=pl.ANY)


def vmem_spec():
    return pl.BlockSpec(memory_space=pltpu.VMEM)


def params(number):
    return pltpu.CompilerParams(collective_id=number, has_side_effects=True, vmem_limit_bytes=VMEM_LIMIT)


def solution(mesh):
    tp, ep = mesh.shape['tp'], mesh.shape['ep']
    dma = pltpu.SemaphoreType.DMA
    token_spec = P(('part', 'ep'), None, None)
    row_spec = P(('part', 'ep'), None)
    col_spec = P(None, 'tp')
    head_rows = P('tp', None)
    vec_spec = P(None)
    expert_spec = P('ep', None, None)
    in_specs = (token_spec, token_spec, row_spec, row_spec, P('tp', None, None), vec_spec, col_spec, col_spec, col_spec, head_rows, vec_spec, col_spec, col_spec, col_spec, head_rows, vec_spec, P(None, None), expert_spec, expert_spec)

    def layer(dec_states, enc_states, enc_pad, expert_idx, self_bias, gain_self, wq_self, wk_self, wv_self, wo_self, gain_cross, wq_cross, wk_cross, wv_cross, wo_cross, gain_ffn, w_router, w_in, w_out):
        seqs, length, width = dec_states.shape
        enc_len = enc_states.shape[1]
        per = seqs // tp
        experts = w_router.shape[1]
        tokens = seqs * length
        cap = (5 * tokens + 4 * experts - 1) // (4 * experts)
        share = experts // ep // tp
        heads = self_bias.shape[0]
        w_self = pack_qkv(wq_self, wk_self, wv_self)
        packed = w_self.shape[1]
        chips = ep // 2
        w_cross = pack_qkv(wq_cross, wk_cross, wv_cross).reshape(2, chips, width // ep, packed)
        wo_both = jnp.concatenate([pack_out(wo_self), pack_out(wo_cross)], axis=0)
        wo_len = wo_both.shape[0]
        wo_both = wo_both.reshape(2, chips, wo_len // ep, width)
        ctx, wq_all, wo_all = pl.pallas_call(
            functools.partial(self_kernel, tp, ep),
            name='self_attend',
            out_shape=(
                jax.ShapeDtypeStruct((tp, per, length, 2 * LANES), BF16),
                jax.ShapeDtypeStruct((tp, *w_cross.shape), BF16),
                jax.ShapeDtypeStruct((tp, *wo_both.shape), BF16),
            ),
            in_specs=[any_spec(), vmem_spec(), vmem_spec(), vmem_spec(), any_spec(), any_spec()],
            out_specs=(any_spec(), any_spec(), any_spec()),
            scratch_shapes=[
                pltpu.VMEM((2, length, width), BF16),
                pltpu.VMEM((6, length, LANES), BF16),
                pltpu.VMEM((seqs, length, 2 * LANES), BF16),
                pltpu.VMEM((2, length, 2 * LANES), BF16),
                pltpu.VMEM(w_cross.shape, BF16),
                pltpu.VMEM(wo_both.shape, BF16),
                dma((2,)), dma((2,)), dma((4, 2)), dma((4, 2)), dma((per,)),
                dma((2, 3)), dma((2, 3)), dma((2, 3, 3)), dma((2, 3, 3)), dma((2, 3)), dma((2, 3)),
            ],
            compiler_params=params(0),
        )(dec_states, gain_self.reshape(1, width), w_self, self_bias, w_cross, wo_both)
        w_all = wq_all.reshape(tp, width, packed)
        wo_all = wo_all.reshape(tp, wo_len, width)
        y2, send, gate, slot = pl.pallas_call(
            functools.partial(cross_kernel, tp, ep, cap, experts),
            name='cross_attend',
            out_shape=(
                jax.ShapeDtypeStruct((seqs, length, width), BF16),
                jax.ShapeDtypeStruct((ep * share * cap, width), BF16),
                jax.ShapeDtypeStruct((length, seqs), F32),
                jax.ShapeDtypeStruct((length, seqs), jnp.int32),
            ),
            in_specs=[vmem_spec(), vmem_spec(), vmem_spec(), any_spec(), any_spec()] + [vmem_spec()] * 6,
            out_specs=(any_spec(), vmem_spec(), vmem_spec(), vmem_spec()),
            scratch_shapes=[
                pltpu.VMEM((per, length, width), BF16),
                pltpu.VMEM((per, enc_len, width), BF16),
                pltpu.VMEM((length, width), BF16),
                pltpu.VMEM((length, width), BF16),
                pltpu.VMEM((3, length, LANES), BF16),
                pltpu.VMEM((3, enc_len, LANES), BF16),
                pltpu.VMEM((length, width), F32),
                pltpu.VMEM((seqs, length, width), BF16),
                pltpu.VMEM((width, 3 * experts), BF16),
                pltpu.VMEM((2, length, length), BF16),
                pltpu.VMEM((seqs, length), jnp.int32),
                dma((per,)), dma((per,)), dma((3, 2)), dma((3, 2)), dma((seqs,)),
            ],
            compiler_params=params(1),
        )(ctx, w_all, wo_all, dec_states, enc_states, enc_pad, gain_cross.reshape(1, width), gain_ffn.reshape(1, width), w_router, expert_idx, expert_idx.T)
        pairs = 2
        rows2 = share // pairs * cap
        return pl.pallas_call(
            functools.partial(expert_kernel, tp, ep, cap),
            name='experts',
            out_shape=jax.ShapeDtypeStruct((seqs, length, width), BF16),
            in_specs=[any_spec(), any_spec(), any_spec(), any_spec(), vmem_spec(), vmem_spec()],
            out_specs=any_spec(),
            scratch_shapes=[
                pltpu.VMEM((ep, pairs, rows2, width), BF16),
                pltpu.VMEM((share, ep * cap, width), F32),
                pltpu.VMEM((rows2, width), F32),
                pltpu.VMEM((pairs, ep, rows2, width), BF16),
                pltpu.VMEM((tp, pairs, ep, rows2, width), BF16),
                pltpu.VMEM((seqs, length, width), BF16),
                pltpu.VMEM((seqs, length, width), BF16),
                pltpu.VMEM((2, width, w_in.shape[2]), BF16),
                pltpu.VMEM((2, w_in.shape[2], width), BF16),
                dma((ep, pairs)), dma((ep, pairs)), dma((ep, pairs)), dma((ep, pairs)),
                dma((4, pairs)), dma((4, pairs)), dma((2, 2)), dma((pairs,)), dma, dma((seqs,)),
            ],
            compiler_params=params(2),
        )(send.reshape(ep, pairs, rows2, width), w_in, w_out, y2, gate, slot)

    return jax.shard_map(layer, mesh=mesh, in_specs=in_specs, out_specs=token_spec, check_vma=False)
```

```python
import functools

import jax
import jax.numpy as jnp
from jax import lax
from jax.experimental import pallas as pl
from jax.experimental.pallas import tpu as pltpu
from jax.sharding import PartitionSpec as P

EPSILON = 1e-6
NEG_LARGE = -1e30
MESH = pl.DeviceIdType.MESH
BF16 = jnp.bfloat16
F32 = jnp.float32
LANES = 128
WIDE = 256
VMEM_LIMIT = 67043328
SIDES = range(2)
ROW = {'axis': -1, 'keepdims': True}
ALL = Ellipsis


def rms_norm(upcast, gain_vec):
    mean_sq = jnp.mean(upcast * upcast, **ROW)
    return (upcast * lax.rsqrt(mean_sq + EPSILON) * gain_vec).astype(BF16)


def dot(a, b):
    return jnp.dot(a, b, preferred_element_type=F32)


def dot_nt(a, b):
    return lax.dot_general(a, b, (((1,), (1,)), ((), ())), preferred_element_type=F32)


def softmax(scores):
    exps = jnp.exp(scores - jnp.max(scores, **ROW))
    return (exps * (1.0 / jnp.sum(exps, **ROW))).astype(BF16)


def low_lanes(rows):
    return lax.broadcasted_iota(jnp.int32, (rows, LANES), 1) < LANES // 2


def pack_qkv(w_query, w_key, w_value, packed):
    half, full = LANES // 2, LANES
    packed[:full + half] = w_query[ALL]
    packed[full + half:2 * full] = jnp.zeros((half, packed.shape[1]), BF16)
    packed[2 * full:3 * full] = w_key[:full]
    packed[3 * full:4 * full] = w_value[:full]
    packed[4 * full:4 * full + half] = w_key[full:]
    packed[4 * full + half:] = w_value[full:]


def remote(src, dst, send_sem, recv_sem, **device):
    return pltpu.make_async_remote_copy(src_ref=src, dst_ref=dst, send_sem=send_sem, recv_sem=recv_sem, device_id=device, device_id_type=MESH)


def greet(devices):
    for device in devices:
        pl.semaphore_signal(pltpu.get_barrier_semaphore(), inc=1, device_id=device, device_id_type=MESH)


def meet(devices):
    pl.semaphore_wait(pltpu.get_barrier_semaphore(), len(devices))


def self_part(tp, ep, dec_ref, gain_ref, bias_ref, wq_self, wk_self, wv_self, wo_self, wq_cross, wk_cross, wv_cross, wo_cross, ctx_ref, wq_all, wo_all, dec_buf, head_buf, ctx_buf, relay, w_ref, dec_sem, ctx_send, ctx_recv, wy_send, wy_recv, wx_send, wx_recv, wd_send, wd_recv):
    t, e = lax.axis_index('tp'), lax.axis_index('ep')
    right, left, across = lax.rem(t + 1, tp), lax.rem(t + tp - 1, tp), lax.rem(t + 2, tp)
    x_right, x_left = lax.rem(e + 2, ep), lax.rem(e + ep - 2, ep)
    chips = ep // 2
    core, x = lax.rem(e, 2), e // 2
    piece = core * chips + x
    piece_left, piece_right = core * chips + x_left // 2, core * chips + x_right // 2
    partner = e + 1 - 2 * core
    seqs, length = dec_ref.shape[0], dec_ref.shape[1]
    per = seqs // tp
    heads = bias_ref.shape[0]
    def seq_at(k):
        off = jnp.where(k < per, 2, jnp.where(k < 2 * per, 1, jnp.where(k < 3 * per, 3, 0)))
        return per * lax.rem(t + off, tp) + lax.rem(k, per)

    def dec_load(k):
        return pltpu.make_async_copy(dec_ref.at[seq_at(k)], dec_buf.at[lax.rem(k, 2)], dec_sem.at[lax.rem(k, 2)])

    dec_load(0).start()
    friends = [{'tp': right}, {'tp': left}, {'tp': across}, {'ep': x_right}, {'ep': x_left}, {'ep': partner}]
    greet(friends)
    pack_qkv(wq_cross, wk_cross, wv_cross, wq_all.at[t])
    wo_all[t, :wo_self.shape[0]] = wo_self[ALL]
    wo_all[t, wo_self.shape[0]:] = wo_cross[ALL]
    meet(friends)
    alls = (wq_all, wo_all)
    rows_of = tuple(buf.shape[1] // ep for buf in alls)

    def rows(a, at):
        return pl.ds(pl.multiple_of(at * rows_of[a], rows_of[a]), rows_of[a])

    def wy_own(a, side):
        src = alls[a].at[t, rows(a, piece)]
        return remote(src, src, wy_send.at[a, side], wy_recv.at[a, side], tp=(right, left)[side])

    def wy_forward(a):
        src = alls[a].at[(left, right)[a], rows(a, piece)]
        return remote(src, src, wy_send.at[a, 2], wy_recv.at[a, 2], tp=(right, left)[a])

    def wx_own(a, which, side):
        src = alls[a].at[(left, right, across)[which], rows(a, piece)]
        return remote(src, src, wx_send.at[a, which, side], wx_recv.at[a, which, side], ep=(x_right, x_left)[side])

    def wx_forward(a, which):
        src = alls[a].at[(left, right, across)[which], rows(a, (piece_left, piece_right)[a])]
        return remote(src, src, wx_send.at[a, which, 2], wx_recv.at[a, which, 2], ep=(x_right, x_left)[a])

    def wd(a, which):
        block_rows = chips * rows_of[a]
        src = alls[a].at[(left, right, across)[which], pl.ds(pl.multiple_of(core * block_rows, block_rows), block_rows)]
        return remote(src, src, wd_send.at[a, which], wd_recv.at[a, which], ep=partner)

    def y_stage():
        for a in SIDES:
            for side in SIDES:
                wy_own(a, side).wait_recv()
            wy_forward(a).start()
        for which in SIDES:
            for a in SIDES:
                for side in SIDES:
                    wx_own(a, which, side).start()

    def across_stage():
        for a in SIDES:
            wy_forward(a).wait_recv()
            for side in SIDES:
                wx_own(a, 2, side).start()

    def x_stage(whichs):
        for which in whichs:
            for a in SIDES:
                for side in SIDES:
                    wx_own(a, which, side).wait_recv()
                wx_forward(a, which).start()

    def d_stage(whichs):
        for which in whichs:
            for a in SIDES:
                wx_forward(a, which).wait_recv()
                wd(a, which).start()

    for a in SIDES:
        for side in SIDES:
            wy_own(a, side).start()
    pack_qkv(wq_self, wk_self, wv_self, w_ref)

    def to_side(i, side):
        return remote(ctx_buf.at[per * (1 + side) + i], ctx_ref.at[t, i], ctx_send.at[side, i], ctx_recv.at[side, i], tp=(right, left)[side])

    def to_relay(side):
        return remote(ctx_buf.at[side], relay.at[side], ctx_send.at[2, side], ctx_recv.at[2, side], tp=(right, left)[side])

    def from_relay(side):
        return remote(relay.at[side], ctx_ref.at[(left, right)[side], side], ctx_send.at[3, side], ctx_recv.at[3, side], tp=(right, left)[side])

    block = length // 2

    def body(k, carry):
        dec_load(k).wait()

        @pl.when(k + 1 < seqs)
        def _():
            dec_load(k + 1).start()

        normed = rms_norm(dec_buf[lax.rem(k, 2)].astype(F32), gain_ref[ALL])
        low = low_lanes(length)
        pair = dot_nt(normed, w_ref[:WIDE])
        q01 = pair[:, :LANES]
        head_buf[0] = jnp.where(low, q01, 0.0).astype(BF16)
        head_buf[1] = jnp.where(low, 0.0, q01).astype(BF16)
        head_buf[2] = pair[:, LANES:].astype(BF16)
        rest = dot_nt(normed, w_ref[WIDE:])
        for piece in range(3):
            head_buf[3 + piece] = rest[:, piece * LANES:(piece + 1) * LANES].astype(BF16)
        low_half = low_lanes(block)
        for half in SIDES:
            span = slice(half * block, (half + 1) * block)
            keys = slice(0, (half + 1) * block)
            row_ids = half * block + lax.broadcasted_iota(jnp.int32, (block, (half + 1) * block), 0)
            col_ids = lax.broadcasted_iota(jnp.int32, (block, (half + 1) * block), 1)
            mixed = []
            for head in range(heads):
                key_at, value_at = (3, 4) if head < 2 else (5, 5)
                scores = dot_nt(head_buf[head, span], head_buf[key_at, keys]) + bias_ref[head, span, keys]
                scores = jnp.where(col_ids <= row_ids, scores, NEG_LARGE)
                mixed.append(dot(softmax(scores), head_buf[value_at, keys]))
            ctx_buf[k, span, :LANES] = jnp.where(low_half, mixed[0], mixed[1]).astype(BF16)
            ctx_buf[k, span, LANES:] = jnp.where(low_half, 0.0, mixed[2]).astype(BF16)

        @pl.when(k == 0)
        def _():
            to_relay(0).start()
            y_stage()

        @pl.when(k == 1)
        def _():
            to_relay(1).start()
            across_stage()

        for side in SIDES:
            for i in range(per):
                @pl.when(k == per * (1 + side) + i)
                def _(side=side, i=i):
                    to_side(i, side).start()

        @pl.when(k == 2)
        def _():
            to_relay(0).wait_recv()
            from_relay(0).start()

        @pl.when(k == 3)
        def _():
            to_relay(1).wait_recv()
            from_relay(1).start()

        @pl.when(k == 3)
        def _():
            x_stage((0, 1))

        @pl.when(k == 4)
        def _():
            x_stage((2,))

        @pl.when(k == 5)
        def _():
            d_stage((0, 1))

        @pl.when(k == 6)
        def _():
            d_stage((2,))

        for i in range(per):
            @pl.when(k == 3 * per + i)
            def _(i=i):
                ctx_ref[t, i] = ctx_buf[3 * per + i]

        return carry

    lax.fori_loop(0, seqs, body, 0)
    for which in range(3):
        for a in SIDES:
            wd(a, which).wait_recv()
    for side in SIDES:
        for i in range(per):
            to_side(i, side).wait_recv()
        from_relay(side).wait_recv()

    def finish():
        for side in SIDES:
            for i in range(per):
                to_side(i, side).wait_send()
            to_relay(side).wait_send()
            from_relay(side).wait_send()
        for a in SIDES:
            for side in SIDES:
                wy_own(a, side).wait_send()
            wy_forward(a).wait_send()
            for which in range(3):
                for side in SIDES:
                    wx_own(a, which, side).wait_send()
                wx_forward(a, which).wait_send()
                wd(a, which).wait_send()

    return finish


def cross_part(tp, ep, cap, experts, finish_self, ctx_ref, w_ref, wo_ref, pad_ref, gain_cross_ref, gain_ffn_ref, router_ref, idx_row_ref, y2_ref, send_ref, gate_ref, place_ref, dec_buf, enc_buf, y1_buf, x_buf, q_buf, kv_buf, acc_buf, y2_buf, route_buf, tri_buf, key_buf, kept_buf, idx_buf, choice_buf, gate_col, gate_out, gate_in, loads, y_send, y_recv, g_send, g_recv, out_sem):
    t, e = lax.axis_index('tp'), lax.axis_index('ep')
    right, left, across = lax.rem(t + 1, tp), lax.rem(t + tp - 1, tp), lax.rem(t + 2, tp)
    seqs, length, width = y2_buf.shape
    per = seqs // tp
    enc_len = enc_buf.shape[1]
    span = experts // ep
    share = span // tp
    chips = ep // 2
    wo_len = wo_ref.shape[1] // 2
    block = y1_buf.shape[0]
    halves = length // block

    def own(i, h, side):
        src = y2_buf.at[per * t + i, pl.ds(h * block, block)]
        return remote(src, src, y_send.at[side, i, h], y_recv.at[side, i, h], tp=(right, left)[side])

    def forward(side, h):
        src = y2_buf.at[per * (left, right)[side] + side, pl.ds(h * block, block)]
        return remote(src, src, y_send.at[2, side, h], y_recv.at[2, side, h], tp=(right, left)[side])

    def gates(side):
        return remote(gate_out, gate_in.at[side], g_send.at[side], g_recv.at[side], tp=(right, left, across)[side])

    def write(s):
        return pltpu.make_async_copy(y2_buf.at[s], y2_ref.at[s], out_sem.at[s])

    low = low_lanes(block)
    for copy in loads:
        copy.wait()

    def keys_values(row, carry):
        rest = dot_nt(enc_buf[ALL].reshape(per * enc_len, width), w_ref[row, WIDE:])
        for piece in range(3):
            kv_buf[row, piece] = rest[:, piece * LANES:(piece + 1) * LANES].astype(BF16)
        return carry

    lax.fori_loop(0, tp, keys_values, 0)
    def attend(step, carry):
        i, h = step // halves, lax.rem(step, halves)
        rows = pl.ds(pl.multiple_of(h * block, block), block)
        total = dec_buf[i, rows, :].astype(F32)
        for row in range(tp):
            total = total + (dot(ctx_ref[row, i, rows, :LANES], wo_ref[row, :LANES]) + dot(ctx_ref[row, i, rows, LANES:], wo_ref[row, wo_len - LANES:wo_len]))
        y1 = total.astype(BF16)
        y1_buf[ALL] = y1
        x_buf[ALL] = rms_norm(y1.astype(F32), gain_cross_ref[ALL])
        acc_buf[ALL] = jnp.zeros_like(acc_buf)
        pad_bias = jnp.where(pad_ref[pl.ds(per * t + i, 1), :] == 0, 0.0, NEG_LARGE)
        keys = pl.ds(pl.multiple_of(i * enc_len, enc_len), enc_len)

        def per_row(row, inner):
            pair = dot_nt(x_buf[ALL], w_ref[row, :WIDE])
            q01 = pair[:, :LANES]
            q_buf[0] = jnp.where(low, q01, 0.0).astype(BF16)
            q_buf[1] = jnp.where(low, 0.0, q01).astype(BF16)
            q_buf[2] = pair[:, LANES:].astype(BF16)
            mixed = []
            for head in range(3):
                key_at, value_at = (0, 1) if head < 2 else (2, 2)
                scores = dot_nt(q_buf[head], kv_buf[row, key_at, keys, :]) + pad_bias
                mixed.append(dot(softmax(scores), kv_buf[row, value_at, keys, :]))
            c01 = jnp.where(low, mixed[0], mixed[1]).astype(BF16)
            c2 = jnp.where(low, 0.0, mixed[2]).astype(BF16)
            acc_buf[ALL] += dot(c01, wo_ref[row, wo_len:wo_len + LANES]) + dot(c2, wo_ref[row, 2 * wo_len - LANES:])
            return inner

        lax.fori_loop(0, tp, per_row, 0)
        y2_buf[per * t + i, rows, :] = (y1_buf[ALL].astype(F32) + acc_buf[ALL]).astype(BF16)
        for at in range(per * halves):
            @pl.when(step == at)
            def _(at=at):
                for side in SIDES:
                    own(at // halves, at % halves, side).start()
        return carry

    lax.fori_loop(0, per * halves, attend, 0)

    w_full = router_ref[ALL]
    w_high = w_full.astype(BF16)
    w_rest = w_full - w_high.astype(F32)
    w_mid = w_rest.astype(BF16)
    route_buf[:, :experts] = w_high
    route_buf[:, experts:2 * experts] = w_mid
    route_buf[:, 2 * experts:] = (w_rest - w_mid.astype(F32)).astype(BF16)
    lane_e = lax.broadcasted_iota(jnp.int32, (length, experts), 1)
    lane_s = lax.broadcasted_iota(jnp.int32, choice_buf.shape, 1)
    idx_buf[ALL] = jnp.zeros_like(idx_buf)
    idx_buf[:seqs] = idx_row_ref[ALL].astype(F32)
    choice_buf[ALL] = idx_buf[ALL].T.astype(jnp.int32)
    gate_col[ALL] = jnp.zeros_like(gate_col)

    def own_gate(i, carry):
        s = per * t + i
        parts = dot(rms_norm(y2_buf[s].astype(F32), gain_ffn_ref[ALL]), route_buf[ALL])
        logits = parts[:, :experts] + (parts[:, experts:2 * experts] + parts[:, 2 * experts:])
        exps = jnp.exp(logits - jnp.max(logits, **ROW))
        choice = jnp.sum(jnp.where(lane_s == s, choice_buf[ALL], 0), **ROW)
        picked = jnp.sum(jnp.where(lane_e == choice, exps, 0.0), **ROW)
        gate_col[ALL] += jnp.where(lane_s == s, picked / jnp.sum(exps, **ROW), 0.0)
        return carry

    lax.fori_loop(0, per, own_gate, 0)
    idx_buf[ALL] = gate_col[ALL].T
    gate_out[ALL] = idx_buf[:seqs]
    for side in range(3):
        gates(side).start()

    row_ids = lax.broadcasted_iota(jnp.int32, (length, length), 0)
    col_ids = lax.broadcasted_iota(jnp.int32, (length, length), 1)
    tri_buf[ALL] = jnp.where(row_ids <= col_ids, 1.0, 0.0).astype(BF16)
    sub_e = lax.broadcasted_iota(jnp.int32, (experts, length), 0)
    first_rows = cap // 16 * 16
    rows2 = share // 2 * cap

    def place(s, base_col):
        row = idx_row_ref[pl.ds(s, 1), :]
        hot_t = jnp.where(sub_e == row, 1.0, 0.0)
        count_t = dot(hot_t.astype(BF16), tri_buf[ALL]) + base_col
        pos_t = jnp.sum(hot_t * count_t, axis=0, keepdims=True) - 1.0
        pos_i = pos_t.astype(jnp.int32)
        kept = pos_t < cap
        home, row_of, at = row // span, lax.rem(row // share, tp), lax.rem(row, share)
        key_buf[pl.ds(s, 1), :] = jnp.where(kept & (row_of == t), home * (share * cap) + at * cap + pos_i, -1)
        away = lax.rem(home // 2 - e // 2 + chips, chips)
        flip = lax.rem(home + e, 2)
        spot = jnp.where(away == 0, flip, jnp.where(away == 1, 2 + flip, jnp.where(away == 2, 6 + flip, 4 + flip)))
        half_share = share // 2
        q = lax.rem(at, half_share) * cap + pos_i
        inside = jnp.where(q < first_rows, spot * first_rows + q, ep * first_rows + spot * (rows2 - first_rows) + q - first_rows)
        where = (row_of * 2 + at // half_share) * (ep * rows2) + inside
        place_ref[pl.ds(s, 1), :] = jnp.where(kept, where * 8, 0)
        kept_buf[pl.ds(s, 1), :] = jnp.where(kept, 1.0, 0.0)
        return count_t[:, length - 1:]

    lax.fori_loop(0, seqs, place, jnp.zeros((experts, 1), F32))
    send_ref[ALL] = jnp.zeros_like(send_ref)
    chunk = send_ref.shape[0] // 2

    def consume(n, carry):
        near = jnp.where(lax.rem(n, 2) == 0, left, right)
        row = jnp.where(n < per, t, jnp.where(n < 3 * per, near, across))
        half = jnp.where(n < per, n, jnp.where(n < 3 * per, lax.rem(n // 2 + 1, 2), lax.rem(n, 2)))
        s = per * row + half

        @pl.when(n == 1)
        def _():
            for h in range(halves):
                own(0, h, 0).wait_recv()
                forward(0, h).start()

        @pl.when(n == 3)
        def _():
            for h in range(halves):
                own(0, h, 1).wait_recv()

        @pl.when(n == 4)
        def _():
            for h in range(halves):
                own(1, h, 1).wait_recv()
                forward(1, h).start()
            for h in range(halves):
                own(1, h, 0).wait_recv()

        for side in SIDES:
            @pl.when(n == 3 * per + side)
            def _(side=side):
                for h in range(halves):
                    forward(side, h).wait_recv()

        write(s).start()

        key = key_buf[pl.ds(s, 1), :]

        def dispatch(d, inner):
            rows = pl.ds(pl.multiple_of(d * chunk, chunk), chunk)
            hot = jnp.where(lax.broadcasted_iota(jnp.int32, (chunk, length), 0) + d * chunk == key, 1.0, 0.0).astype(BF16)
            send_ref[rows, :] = (send_ref[rows, :].astype(F32) + dot(hot, y2_buf[s])).astype(BF16)
            return inner

        lax.fori_loop(0, 2, dispatch, 0)
        return carry

    lax.fori_loop(0, seqs, consume, 0)
    finish_self()
    for side in range(3):
        gates(side).wait()
    gate_ref[ALL] = (gate_out[ALL] + gate_in[0] + gate_in[1] + gate_in[2]) * kept_buf[ALL]
    for s in range(seqs):
        write(s).wait()
    for side in SIDES:
        for h in range(halves):
            for i in range(per):
                own(i, h, side).wait_send()
            forward(side, h).wait_send()


def attention_kernel(tp, ep, cap, experts, dec_ref, enc_ref, pad_ref, idx_ref, bias_ref, gain_self, gain_cross, gain_ffn, router_ref, wq_self, wk_self, wv_self, wo_self, wq_cross, wk_cross, wv_cross, wo_cross, y2_ref, send_ref, gate_ref, place_ref, ctx_all, w_all, wo_all, dec_pair, head_buf, ctx_buf, relay, w_ref, dec_buf, enc_buf, y1_buf, x_buf, q_buf, kv_buf, acc_buf, y2_buf, route_buf, tri_buf, key_buf, kept_buf, idx_buf, choice_buf, gate_col, gate_out, gate_in, dec_sem, ctx_send, ctx_recv, wy_send, wy_recv, wx_send, wx_recv, wd_send, wd_recv, load_sem, y_send, y_recv, g_send, g_recv, out_sem):
    per = dec_buf.shape[0]
    t = lax.axis_index('tp')
    finish_self = self_part(tp, ep, dec_ref, gain_self, bias_ref, wq_self, wk_self, wv_self, wo_self, wq_cross, wk_cross, wv_cross, wo_cross, ctx_all, w_all, wo_all, dec_pair, head_buf, ctx_buf, relay, w_ref, dec_sem, ctx_send, ctx_recv, wy_send, wy_recv, wx_send, wx_recv, wd_send, wd_recv)
    loads = [
        pltpu.make_async_copy(enc_ref.at[pl.ds(per * t, per)], enc_buf, load_sem.at[0]),
        pltpu.make_async_copy(dec_ref.at[pl.ds(per * t, per)], dec_buf, load_sem.at[1]),
    ]
    for copy in loads:
        copy.start()
    cross_part(tp, ep, cap, experts, finish_self, ctx_all, w_all, wo_all, pad_ref, gain_cross, gain_ffn, router_ref, idx_ref, y2_ref, send_ref, gate_ref, place_ref, dec_buf, enc_buf, y1_buf, x_buf, q_buf, kv_buf, acc_buf, y2_buf, route_buf, tri_buf, key_buf, kept_buf, idx_buf, choice_buf, gate_col, gate_out, gate_in, loads, y_send, y_recv, g_send, g_recv, out_sem)


def expert_kernel(tp, ep, cap, send_ref, w_in_ref, w_out_ref, gain_ref, all_hbm, all_ref, got, relay, staged, acc_buf, out_stage, out_buf, back, w_in_buf, w_out_buf, xd_send, xd_recv, xr_send, xr_recv, y_send, y_recv, w_sem, own_sem, out_sem):
    t, e = lax.axis_index('tp'), lax.axis_index('ep')
    right, left, across = lax.rem(t + 1, tp), lax.rem(t + tp - 1, tp), lax.rem(t + 2, tp)
    chips = ep // 2
    core, x = lax.rem(e, 2), e // 2
    share, _, width = staged.shape
    ff = w_in_buf.shape[2]
    rows2 = 2 * cap
    over, under = (cap + 15) // 16 * 16, cap // 16 * 16
    in_at = tuple(j // 2 * rows2 + j % 2 * over for j in range(share))
    in_len = tuple((rows2 - over) if j % 2 else over for j in range(share))
    out_at = tuple(j // 2 * rows2 + j % 2 * under for j in range(share))
    out_len = tuple((rows2 - under) if j % 2 else under for j in range(share))

    def inn(j):
        return pl.ds(in_at[j], in_len[j])

    def out(j):
        return pl.ds(out_at[j], out_len[j])

    def region(j, n, count=1):
        return pl.ds(out_at[j] * ep + n * out_len[j], count * out_len[j])

    def member(dx, flip):
        return 2 * lax.rem(x + dx + chips, chips) + (core if flip == 0 else 1 - core)

    near = {1: (0, 1), 2: (1, 0), 3: (1, 1), 4: (-1, 0), 5: (-1, 1)}
    x_right, x_left = member(1, 0), member(-1, 0)
    friends = [{'tp': right}, {'tp': left}] + [{'ep': member(*near[n])} for n in near]
    greet(friends)

    def to(n):
        return member(*near[n])

    def origin(n):
        return e if n == 0 else member(-near[n][0], near[n][1]) if n in near else member(2, n - 6)

    def dispatch(n, j):
        return remote(send_ref.at[to(n), inn(j)], got.at[n, inn(j)], xd_send.at[n, j], xd_recv.at[n, j], ep=to(n))

    def dispatch_via(side, j):
        return remote(send_ref.at[member(2, side), inn(j)], relay.at[side, inn(j)], xd_send.at[6 + side, j], xd_recv.at[6 + side, j], ep=(x_right, x_left)[side])

    def dispatch_on(side, j):
        return remote(relay.at[side, inn(j)], got.at[6 + side, inn(j)], xd_send.at[8 + side, j], xd_recv.at[8 + side, j], ep=(x_right, member(-1, 1))[side])

    def give(n, j):
        return remote(out_buf.at[n, out(j)], all_ref.at[t, region(j, n)], xr_send.at[n, j], xr_recv.at[n, j], ep=origin(n))

    def give_via(side, j):
        return remote(out_buf.at[6 + side, out(j)], back.at[side, out(j)], xr_send.at[6 + side, j], xr_recv.at[6 + side, j], ep=(x_right, x_left)[side])

    def give_on(side, j):
        return remote(back.at[side, out(j)], all_ref.at[t, region(j, 6 + side)], xr_send.at[8 + side, j], xr_recv.at[8 + side, j], ep=(x_right, member(-1, 1))[side])

    def own_dispatch(j):
        return pltpu.make_async_copy(send_ref.at[e, inn(j)], got.at[0, inn(j)], own_sem.at[0, j])

    def write(r, j):
        row = (t, left, right, across)[r]
        return pltpu.make_async_copy(all_ref.at[row, region(j, 0, ep)], all_hbm.at[row, region(j, 0, ep)], out_sem.at[r, j])

    def weights(j):
        return (pltpu.make_async_copy(w_in_ref.at[share * t + j], w_in_buf.at[j], w_sem.at[0, j]), pltpu.make_async_copy(w_out_ref.at[share * t + j], w_out_buf.at[j], w_sem.at[1, j]))

    def dispatch_all(j):
        for side in SIDES:
            dispatch_via(side, j).start()
        for n in (2, 4, 3, 5, 1):
            dispatch(n, j).start()
        own_dispatch(j).start()

    def unpack(n, j):
        start = j // 2 * rows2 + (under if j % 2 else 0)
        block = got[n, start:start + over].astype(F32)
        block = block[over - cap:] if j % 2 else block[:cap]
        staged[j, n * cap:(n + 1) * cap, :] = rms_norm(block, gain_ref[ALL]).astype(F32)

    def run_expert(j):
        for copy in weights(j):
            copy.wait()
        inputs = staged[j].astype(BF16)

        def ffn(c, carry):
            cols = pl.ds(pl.multiple_of(c * width, LANES), width)
            hidden = jnp.maximum(dot(inputs, w_in_buf[j, :, cols]), 0.0).astype(BF16)
            acc = dot(hidden, w_out_buf[j, cols, :])

            @pl.when(c == 0)
            def _():
                acc_buf[j % 2] = acc

            @pl.when(c > 0)
            def _():
                acc_buf[j % 2] += acc

            return carry

        lax.fori_loop(0, ff // width, ffn, 0)

    def repack(n, j):
        start = n * cap
        if j % 2 == 0:
            out_buf[n, out_at[j]:out_at[j] + under] = acc_buf[0, start:start + under].astype(BF16)
        else:
            out_stage[:cap - under] = acc_buf[0, start + under:start + cap]
            out_stage[cap - under:] = acc_buf[1, start:start + cap]
            out_buf[n, out_at[j]:out_at[j] + out_len[j]] = out_stage[ALL].astype(BF16)

    def dispatch_forward(j):
        for side in SIDES:
            dispatch_via(side, j).wait_recv()
            dispatch_on(side, j).start()

    def forward_back(j):
        for side in SIDES:
            give_via(side, j).wait_recv()
            give_on(side, j).start()

    def take(j):
        own_dispatch(j).wait()
        unpack(0, j)
        for n in (1, 2, 4, 3, 5):
            dispatch(n, j).wait_recv()
            unpack(n, j)
        for side in SIDES:
            dispatch_on(side, j).wait_recv()
            unpack(6 + side, j)

    def give_all(j):
        for n in (6, 7, 2, 4, 3, 5, 1, 0):
            repack(n, j)
            if n >= 6:
                give_via(n - 6, j).start()
            elif n > 0:
                give(n, j).start()
            else:
                all_ref[t, region(j, 0)] = out_buf[0, out_at[j]:out_at[j] + out_len[j]]

    parts = ((0, 2), (2, 4), (6, 2))

    def share_out(c, j, side):
        src = all_ref.at[t, region(j, *parts[c])]
        return remote(src, src, y_send.at[side, c, j], y_recv.at[side, c, j], tp=(right, left)[side])

    def pass_on(side, j):
        src = all_ref.at[(left, right)[side], region(j, side * chips, chips)]
        return remote(src, src, y_send.at[2, side, j], y_recv.at[2, side, j], tp=(right, left)[side])

    def broadcast(j, chosen=(0, 1, 2)):
        for c in chosen:
            for n in ((0, 1), (2, 4, 3, 5), (6, 7))[c]:
                if 0 < n < 6:
                    give(n, j).wait_recv()
                elif n >= 6:
                    give_on(n - 6, j).wait_recv()
            for side in SIDES:
                share_out(c, j, side).start()

    def relay_out(j):
        for c in SIDES:
            for side in SIDES:
                share_out(c, j, side).wait_recv()
        pass_on(0, j).start()
        for side in SIDES:
            share_out(2, j, side).wait_recv()
        pass_on(1, j).start()
        for r in range(3):
            write(r, j).start()

    def collect(j):
        for side in SIDES:
            pass_on(side, j).wait_recv()
        write(3, j).start()

    def fetch(j):
        for copy in weights(j):
            copy.start()

    def early(j):
        broadcast(j, SIDES)

    def late(j):
        broadcast(j, (len(parts) - 1,))

    a, b, c, d = range(share)
    fetch(a)
    meet(friends)
    for j in (a, b, c, d):
        dispatch_all(j)
    for j in (b, c, d):
        fetch(j)
    dispatch_forward(a)
    take(a)
    run_expert(a)
    dispatch_forward(b)
    dispatch_forward(c)
    give_all(a)
    take(b)
    run_expert(b)
    dispatch_forward(d)
    forward_back(a)
    give_all(b)
    early(a)
    take(c)
    run_expert(c)
    forward_back(b)
    late(a)
    give_all(c)
    early(b)
    relay_out(a)
    take(d)
    run_expert(d)
    late(b)
    forward_back(c)
    give_all(d)
    early(c)
    late(c)
    relay_out(b)
    forward_back(d)
    early(d)
    late(d)
    relay_out(c)
    collect(a)
    collect(b)
    relay_out(d)
    collect(c)
    collect(d)
    for j in range(share):
        for side in SIDES:
            pass_on(side, j).wait_send()
            for c in range(len(parts)):
                share_out(c, j, side).wait_send()
            dispatch_via(side, j).wait_send()
            dispatch_on(side, j).wait_send()
            give_via(side, j).wait_send()
            give_on(side, j).wait_send()
        for n in near:
            dispatch(n, j).wait_send()
            give(n, j).wait_send()
        for r in range(tp):
            write(r, j).wait()


def combine_kernel(place_ref, all_ref, y2_ref, gate_ref, out_ref, raw, wide, picked, gate_pad, gate_col, raw_sem):
    s = pl.program_id(0)
    blocks, rows, width = raw.shape
    tiles = width // LANES
    length = picked.shape[0] // 8

    @pl.when(s == 0)
    def _():
        def load(b):
            return pltpu.make_async_copy(all_ref.at[b], raw.at[b], raw_sem.at[b])

        for b in range(blocks):
            load(b).start()
        gate_pad[ALL] = jnp.zeros_like(gate_pad)
        gate_pad[:gate_ref.shape[0]] = gate_ref[ALL]
        gate_col[ALL] = gate_pad[ALL].T

        def spread(b, carry):
            load(b).wait()

            def part(i, inner):
                values = raw[b, pl.ds(pl.multiple_of(i * 16, 16), 16), :].astype(F32)
                start = pl.multiple_of((b * rows + i * 16) * 8, LANES)
                for j in range(tiles):
                    wide[pl.ds(start + j, 16, stride=8), :] = values[:, j * LANES:(j + 1) * LANES]
                return inner

            lax.fori_loop(0, rows // 16, part, 0, unroll=4)
            return carry

        lax.fori_loop(0, blocks, spread, 0)

    def pick(i, carry):
        for u in range(16):
            token = i * 16 + u
            start = pl.multiple_of(place_ref[s, token], 8)
            picked[pl.ds(pl.multiple_of(token * 8, 8), 8), :] = wide[pl.ds(start, 8), :]
        return carry

    lax.fori_loop(0, length // 16, pick, 0)
    lane_s = lax.broadcasted_iota(jnp.int32, gate_col.shape, 1)
    gate = jnp.sum(jnp.where(lane_s == s, gate_col[ALL], 0.0), **ROW)
    for j in range(tiles):
        cols = slice(j * LANES, (j + 1) * LANES)
        out_ref[0, :, cols] = (y2_ref[0, :, cols].astype(F32) + gate * picked[pl.ds(j, length, stride=8), :]).astype(BF16)


def any_spec():
    return pl.BlockSpec(memory_space=pl.ANY)


def vmem_spec():
    return pl.BlockSpec(memory_space=pltpu.VMEM)


def params(number):
    return pltpu.CompilerParams(collective_id=number, has_side_effects=True, vmem_limit_bytes=VMEM_LIMIT)


def solution(mesh):
    tp, ep = mesh.shape['tp'], mesh.shape['ep']
    dma = pltpu.SemaphoreType.DMA
    token_spec = P(('part', 'ep'), None, None)
    row_spec = P(('part', 'ep'), None)
    col_spec = P(None, 'tp')
    head_rows = P('tp', None)
    vec_spec = P(None)
    expert_spec = P('ep', None, None)
    in_specs = (token_spec, token_spec, row_spec, row_spec, P('tp', None, None), vec_spec, col_spec, col_spec, col_spec, head_rows, vec_spec, col_spec, col_spec, col_spec, head_rows, vec_spec, P(None, None), expert_spec, expert_spec)

    def layer(dec_states, enc_states, enc_pad, expert_idx, self_bias, gain_self, wq_self, wk_self, wv_self, wo_self, gain_cross, wq_cross, wk_cross, wv_cross, wo_cross, gain_ffn, w_router, w_in, w_out):
        seqs, length, width = dec_states.shape
        enc_len = enc_states.shape[1]
        per = seqs // tp
        experts = w_router.shape[1]
        tokens = seqs * length
        cap = (5 * tokens + 4 * experts - 1) // (4 * experts)
        share = experts // ep // tp
        two, six = dma((2,)), dma((2, 3))
        packed, out_rows = 5 * LANES, 2 * wo_self.shape[0]
        y2, send, gate, place = pl.pallas_call(
            functools.partial(attention_kernel, tp, ep, cap, experts),
            name='attention',
            out_shape=(
                jax.ShapeDtypeStruct((seqs, length, width), BF16),
                jax.ShapeDtypeStruct((ep * share * cap, width), BF16),
                jax.ShapeDtypeStruct((seqs, length), F32),
                jax.ShapeDtypeStruct((seqs, length), jnp.int32),
            ),
            in_specs=[any_spec(), any_spec()] + [vmem_spec()] * 15,
            out_specs=(any_spec(), vmem_spec(), vmem_spec(), vmem_spec()),
            scratch_shapes=[
                pltpu.VMEM((tp, per, length, WIDE), BF16),
                pltpu.VMEM((tp, packed, width), BF16),
                pltpu.VMEM((tp, out_rows, width), BF16),
                pltpu.VMEM((2, length, width), BF16),
                pltpu.VMEM((6, length, LANES), BF16),
                pltpu.VMEM((seqs, length, WIDE), BF16),
                pltpu.VMEM((2, length, WIDE), BF16),
                pltpu.VMEM((packed, width), BF16),
                pltpu.VMEM((per, length, width), BF16),
                pltpu.VMEM((per, enc_len, width), BF16),
                pltpu.VMEM((length // 2, width), BF16),
                pltpu.VMEM((length // 2, width), BF16),
                pltpu.VMEM((3, length // 2, LANES), BF16),
                pltpu.VMEM((tp, 3, per * enc_len, LANES), BF16),
                pltpu.VMEM((length // 2, width), F32),
                pltpu.VMEM((seqs, length, width), BF16),
                pltpu.VMEM((width, 3 * experts), BF16),
                pltpu.VMEM((length, length), BF16),
                pltpu.VMEM((seqs, length), jnp.int32),
                pltpu.VMEM((seqs, length), F32),
                pltpu.VMEM((LANES, length), F32),
                pltpu.VMEM((length, LANES), jnp.int32),
                pltpu.VMEM((length, LANES), F32),
                pltpu.VMEM((seqs, length), F32),
                pltpu.VMEM((3, seqs, length), F32),
                two, *[dma((4, 2))] * 2, *[six] * 2, *[dma((2, 3, 3))] * 2, *[six] * 2, two, *[dma((3, per, 2))] * 2, *[dma((3,))] * 2, dma((seqs,)),
            ],
            compiler_params=params(0),
        )(dec_states, enc_states, enc_pad, expert_idx, self_bias, gain_self, gain_cross, gain_ffn, w_router, wq_self.T, wk_self.T, wv_self.T, wo_self, wq_cross.T, wk_cross.T, wv_cross.T, wo_cross)
        ff = w_in.shape[2]
        rows = share * cap
        expert_out = pl.pallas_call(
            functools.partial(expert_kernel, tp, ep, cap),
            name='experts',
            out_shape=jax.ShapeDtypeStruct((tp, ep * rows, width), BF16),
            in_specs=[any_spec(), any_spec(), any_spec(), vmem_spec()],
            out_specs=any_spec(),
            scratch_shapes=[
                pltpu.VMEM((tp, ep * rows, width), BF16),
                pltpu.VMEM((ep, rows, width), BF16),
                pltpu.VMEM((2, rows, width), BF16),
                pltpu.VMEM((share, ep * cap, width), F32),
                pltpu.VMEM((2, ep * cap, width), F32),
                pltpu.VMEM((2 * cap - cap // 16 * 16, width), F32),
                pltpu.VMEM((ep, rows, width), BF16),
                pltpu.VMEM((2, rows, width), BF16),
                pltpu.VMEM((share, width, ff), BF16),
                pltpu.VMEM((share, ff, width), BF16),
                *[dma((ep + 2, share))] * 4, *[dma((3, 3, share))] * 2, *[dma((2, share))] * 2, dma((tp, share)),
            ],
            compiler_params=params(2),
        )(send.reshape(ep, rows, width), w_in, w_out, gain_ffn)
        slots = tp * ep * rows
        blocks = 2 * tp
        return pl.pallas_call(
            combine_kernel,
            name='combine',
            grid=(seqs,),
            out_shape=jax.ShapeDtypeStruct((seqs, length, width), BF16),
            in_specs=[
                pl.BlockSpec(memory_space=pltpu.SMEM),
                any_spec(),
                pl.BlockSpec((1, length, width), lambda s: (s, 0, 0)),
                vmem_spec(),
            ],
            out_specs=pl.BlockSpec((1, length, width), lambda s: (s, 0, 0)),
            scratch_shapes=[
                pltpu.VMEM((blocks, slots // blocks, width), BF16),
                pltpu.VMEM((slots * 8, LANES), F32),
                pltpu.VMEM((length * 8, LANES), F32),
                pltpu.VMEM((LANES, length), F32),
                pltpu.VMEM((length, LANES), F32),
                dma((blocks,)),
            ],
            compiler_params=pltpu.CompilerParams(vmem_limit_bytes=VMEM_LIMIT),
        )(place, expert_out.reshape(blocks, slots // blocks, width), y2, gate)

    return jax.shard_map(layer, mesh=mesh, in_specs=in_specs, out_specs=token_spec, check_vma=False)
```
